512 devices in a mesh: depth: 4 (over y_hi, core), blk: 128 (over z, x, y_lo).
Axes of the slice: x: 4, y: 4 (y_hi: 2, y_lo: 2; y = y_hi * 2 + y_lo), z: 16, core: 2. Of those that a mesh axis runs over, the one named last changes fastest.
Arguments:
- jacobian: bfloat16 [1536, 16384], P(('depth', 'blk')), may hold values from -6 to 6
- gain_inverse: bfloat16 [16384, 16384], P('depth', 'blk'), may hold values from -0.00024414062 to 0.00048828125, as said below
- variance: float32 [1536], P(('depth', 'blk')), may hold values from 2 to 12
Outputs:
- omega_diag: float32 [1536], P(('depth', 'blk'))
The draws below stay inside these ranges and needn't reach their ends.
Inputs may be any that keep to these rules, and one draw needn't show every extreme that they name: gain_inverse is symmetric and positive definite.
All inputs are finite; a program needn't handle non-finite values.
Results may differ from the reference program's by a relative error of at most 0.0003.
Values may be sent and summed in bfloat16 or wider, within the bound.
A program may use at most 128 MiB of HBM per device.

```python
import math
import jax
import jax.numpy as jnp

S = 16384
M = 1536


def draw_gain_inverse(key, part):
    noise_key = jax.random.fold_in(key, 11)
    gains_key = jax.random.fold_in(key, 23)
    gains = jnp.exp(jax.random.uniform(gains_key, (S,), jnp.float32, jnp.log(0.6), jnp.log(1.6)))
    noise = jax.random.normal(noise_key, (S, S), jnp.float32)
    places = jnp.arange(S).astype(jnp.float32)
    distance = jnp.abs(places[:, None] - places[None, :])
    kernel = jnp.exp(-distance / (S / 4.0))
    ident = (distance == 0.0).astype(jnp.float32)
    rough = (noise + noise.T) * (0.4 / jnp.sqrt(2.0 * S))
    matrix = gains[:, None] * gains[None, :] * (ident + kernel + rough) / (2.0 * S)
    return matrix.astype(jnp.bfloat16)


def block_levels(own_key, dims, split, low, top_value):
    factor_of, own = 1.0, jax.random.fold_in(own_key, 6)
    for axis_at, parts in split:
        heights = jnp.exp(jax.random.uniform(jax.random.fold_in(own, axis_at), (parts,), jnp.float32, low / len(split), top_value / len(split)))
        factor_of = factor_of * jnp.repeat(heights, dims[axis_at] // parts).reshape([-1 if axis == axis_at else 1 for axis in range(len(dims))])
    return factor_of


def bell_draw(rng, extent, scale, reach, split=(), kind=jnp.bfloat16):
    drawn = jax.random.normal(rng, extent, jnp.float32) * scale
    if len(split) > 0:
        drawn = block_levels(rng, extent, split, -0.22, 0.18) * drawn
    return jnp.clip(drawn, min=-reach, max=reach).astype(kind)


def setup_inputs(seed: int = 0) -> dict:
    seeds = jax.random.split(jax.random.key(seed), 4)
    jacobian = bell_draw(seeds[0], (M, S), 1.0, 6.0, ((0, 512),))
    gain_inverse = draw_gain_inverse(jax.random.fold_in(seeds[3], 71), 0)
    variance = jnp.clip(jnp.exp(math.log(12.0) - 1.7917595 * jax.random.uniform(seeds[2], (M,), jnp.float32) ** block_levels(seeds[2], (M,), ((0, 512),), -0.2, 0.2)), 2.0, 12.0)
    return {"jacobian": jacobian, "gain_inverse": gain_inverse, "variance": variance}


def reference(jacobian, gain_inverse, variance):
    projected = jnp.dot(jacobian, gain_inverse, preferred_element_type=jnp.float32)
    quadratic = jnp.sum(projected * jacobian.astype(jnp.float32), axis=1)
    return variance - quadratic
```

```python
import functools

import jax
import jax.numpy as jnp
from jax import lax
from jax.experimental import pallas as pl
from jax.experimental.pallas import tpu as pltpu
from jax.sharding import Mesh
from jax.sharding import PartitionSpec as P

AXES = ("yh", "c", "z", "x", "yl")
MESH = pl.DeviceIdType.MESH
SUBS = 6
NP = 16


def place(p):
    return {"x": p // 4, "yh": (p // 2) % 2, "yl": p % 2}


def kernel(
    nz, rows, jac, var, g, out, fa, fb, ja, jb, ra, rb, ap, ap2, bp, g2, cc, perm, qs, r1, s2, r2,
    p1_send, p1_recv, g_send, g_recv, d_sem, ring_send, ring_recv, a_send, a_recv,
    ad_send, ad_recv, bd_send, bd_recv, q_send, q_recv,
):
    chunk = NP * rows
    both = 2 * chunk
    c = lax.axis_index("c")
    z = lax.axis_index("z")
    x = lax.axis_index("x")
    yh = lax.axis_index("yh")
    yl = lax.axis_index("yl")
    y = 2 * yh + yl
    w = 4 * x + y
    half = g2.shape[0] // 2
    wide = g2.shape[1] // 8
    own = 2 * x + yl

    def remote(src, dst, send, recv, device):
        return pltpu.make_async_remote_copy(
            src_ref=src, dst_ref=dst, send_sem=send, recv_sem=recv, device_id=device, device_id_type=MESH
        )

    barrier = pltpu.get_barrier_semaphore()

    @pl.loop(1, nz)
    def _(i):
        for core in range(2):
            pl.semaphore_signal(barrier, inc=1, device_id={"z": (z + i) % nz, "c": core}, device_id_type=MESH)

    @pl.loop(1, NP)
    def _(i):
        for core in range(2):
            to = dict(place((w + i) % NP), c=core)
            pl.semaphore_signal(barrier, inc=1, device_id=to, device_id_type=MESH)

    pl.semaphore_signal(barrier, inc=1, device_id={"c": 1 - c}, device_id_type=MESH)
    own_g = pltpu.make_async_copy(
        g.at[pl.ds(pl.multiple_of(own * half, half), half), :],
        g2.at[pl.ds(pl.multiple_of(c * half, half), half), pl.ds(pl.multiple_of(own * wide, wide), wide)],
        d_sem.at[2],
    )
    own_g.start()

    with jax.named_scope("prep"):
        for b in range(8 * nz):
            tile = jac[:, b * 128 : (b + 1) * 128].astype(jnp.float32)
            fa[b * rows : (b + 1) * rows, :] = tile
            rest, k = divmod(b, 4)
            rest, bl = divmod(rest, 2)
            rest, bx = divmod(rest, 4)
            byh, h = divmod(rest, 2)
            to = ((4 * bx + 2 * byh + bl) * 2 + h) * 4 + k
            fb[to * rows : (to + 1) * rows, :] = tile
        ja[...] = fa[...].reshape(ja.shape).astype(jnp.bfloat16)
        jb[...] = fb[...].reshape(jb.shape).astype(jnp.bfloat16)

    with jax.named_scope("barrier"):
        pl.semaphore_wait(barrier, 2 * (nz + NP - 2) + 1)

    def first_b(p):
        return remote(jb.at[p], rb.at[c, w], p1_send.at[0, p], p1_recv.at[c, w], dict(place(p), c=1))

    def first_a(p):
        return remote(ja.at[p], ra.at[c, z], p1_send.at[1, p], p1_recv.at[c, z], {"z": p, "c": 0})

    @pl.loop(1, NP)
    def _(i):
        first_b((w + i) % NP).start()

    @pl.loop(1, nz)
    def _(i):
        first_a((z + i) % nz).start()

    @pl.when(c == 0)
    def _():
        first_b(w).start()
        ra[0, z] = ja[z]

    @pl.when(c == 1)
    def _():
        first_a(z).start()
        rb[1, w] = jb[w]

    def g_copy(p, source):
        return remote(
            g.at[pl.ds(pl.multiple_of(p * half, half), half), :],
            g2.at[pl.ds(pl.multiple_of(c * half, half), half), pl.ds(pl.multiple_of(source * wide, wide), wide)],
            g_send.at[p], g_recv.at[source], {"x": p // 2, "yl": p % 2},
        )

    @pl.loop(1, 8)
    def _(i):
        g_copy((own + i) % 8, own).start()

    def third(v):
        return lax.shift_right_logical(v * 21846, 16)

    def by_chunk(v):
        return lax.shift_right_logical(v * 1366, 16)

    n = 8 * chunk
    oi = lax.broadcasted_iota(jnp.int32, (n, n), 0)
    oj = lax.broadcasted_iota(jnp.int32, (n, n), 1)
    ki = by_chunk(oi)
    mi = oi - chunk * ki
    ti = third(mi)
    q_of = (oj == ti * (8 * rows) + ki * rows + (mi - 3 * ti)).astype(jnp.float32).astype(jnp.bfloat16)

    total = nz * chunk

    @pl.loop(0, nz)
    def _(k):
        mi = lax.broadcasted_iota(jnp.int32, (chunk, total), 0)
        mj = lax.broadcasted_iota(jnp.int32, (chunk, total), 1)
        ti = third(mi)
        hit = mj == ti * (nz * rows) + k * rows + (mi - 3 * ti)
        perm[pl.ds(pl.multiple_of(k * chunk, chunk), chunk), :] = hit.astype(jnp.float32).astype(jnp.bfloat16)

    def repack(src, dst):
        for core in range(2):
            flat = src[core].reshape(n, 128)
            packed = jnp.dot(q_of, flat, preferred_element_type=jnp.float32).astype(jnp.bfloat16)
            for k in range(8):
                dst[core * chunk : (core + 1) * chunk, k * 128 : (k + 1) * 128] = packed[k * chunk : (k + 1) * chunk]

    sub = both // SUBS
    far = nz // 2

    def source_of(way, step):
        return (z + nz - step) % nz if way == 0 else (z + step) % nz

    def ring(way, step, s):
        ref = bp.at[source_of(way, step), pl.ds(s * sub, sub), :]
        to = (z + 1) % nz if way == 0 else (z + nz - 1) % nz
        return ref, to

    def ring_copy(way, step, s):
        ref, to = ring(way, step, s)
        return remote(ref, ref, ring_send.at[way, step, s], ring_recv.at[way, step, s], {"z": to})

    def ring_landed(way, step, s):
        ref, to = ring(way, step, s)
        return remote(ref, ref, ring_send.at[way, step - 1, s], ring_recv.at[way, step - 1, s], {"z": to})

    def goes(way, step, s):
        return step < far or (s < SUBS // 2) == (way == 0)

    def b_across(source):
        ref = bp.at[source, pl.ds(0, chunk), :]
        return remote(ref, ref, bd_send.at[source], bd_recv.at[source], {"c": 1 - c})

    def ring_step(step):
        for s in range(SUBS):
            for way in range(2):
                if step > 0 and goes(way, step, s):
                    ring_landed(way, step, s).wait_recv()
                if step < far and goes(way, step + 1, s):
                    ring_copy(way, step, s).start()
                last = s == SUBS // 2 - 1
                if last and step > 0 and goes(way, step, s):
                    b_across(source_of(way, step)).start()

    lanes = ap.shape[3] // 2

    def unit(kind, source, r0, nr):
        if kind == 0:
            return ap.at[source, y, pl.ds(r0, nr), pl.ds(0, lanes)]
        if kind == 1:
            return ap.at[x, source, pl.ds(r0, nr), pl.ds(lanes, lanes)]
        if kind == 2:
            return ap.at[:, source, pl.ds(r0, nr), pl.ds(0, lanes)]
        return ap.at[source, :, pl.ds(r0, nr), pl.ds(lanes, lanes)]

    def mover(kind, way, hop, source):
        at = x if kind in (0, 3) else y
        to = (at + 1) % 4 if way == 0 else (at + 3) % 4
        device = {"x": to} if kind in (0, 3) else {"yh": to // 2, "yl": to % 2}
        ref = unit(kind, source, 0, both) if hop == 0 else unit(kind, source, way * chunk, chunk)
        return remote(ref, ref, a_send.at[kind, way, hop], a_recv.at[kind, way, hop], device)

    def a_across(kind, source):
        ref = unit(kind, source, chunk, chunk)
        return remote(ref, ref, ad_send.at[kind - 2, source], ad_recv.at[kind - 2, source], {"c": 1 - c})

    def four(kind, stage):
        at = x if kind in (0, 3) else y
        if stage == 0 and kind > 1:
            a_across(kind, at).start()
        for way in range(2):
            behind = (at + 3) % 4 if way == 0 else (at + 1) % 4
            if stage == 0:
                mover(kind, way, 0, at).start()
            elif stage == 1:
                mover(kind, way, 0, behind).wait_recv()
                mover(kind, way, 1, behind).start()
                if kind > 1:
                    a_across(kind, behind).start()
            else:
                mover(kind, way, 1, (at + 2) % 4).wait_recv()
        if stage == 2 and kind > 1:
            a_across(kind, (at + 2) % 4).start()

    mine = g2.at[pl.ds(pl.multiple_of(c * half, half), half), :]
    theirs = g2.at[pl.ds(pl.multiple_of((1 - c) * half, half), half), :]
    across = remote(mine, mine, d_sem.at[0], d_sem.at[1], {"c": 1 - c})

    def g_pass():
        with jax.named_scope("g_wait"):
            own_g.wait()

            @pl.loop(1, 8)
            def _(i):
                p = (own + i) % 8
                g_copy(p, p).wait_recv()

            across.start()

    def g_whole():
        with jax.named_scope("g_across"):
            remote(theirs, theirs, d_sem.at[0], d_sem.at[1], {"c": 1 - c}).wait_recv()

    blocks = g2.shape[0] // 256

    def permute():
        with jax.named_scope("permute"):

            @pl.loop(0, blocks)
            def _(k):
                cols = pl.ds(pl.multiple_of(k * 256, 256), 256)
                whole = ap[:, :, pl.ds(pl.multiple_of(c * chunk, chunk), chunk), cols].reshape(total, 256)
                ap2[:, cols] = jnp.dot(perm[...], whole, preferred_element_type=jnp.float32).astype(jnp.bfloat16)

    def multiply():
        with jax.named_scope("multiply"):

            @pl.loop(0, blocks)
            def _(k):
                cols = pl.ds(pl.multiple_of(k * 256, 256), 256)
                cc[:, cols] = lax.dot_general(
                    ap2[...], g2[cols, :], (((1,), (1,)), ((), ())), preferred_element_type=jnp.float32
                )

    ones = jnp.ones((8, 128), jnp.float32)

    def part(source):
        panel = bp[source, pl.ds(pl.multiple_of(c * chunk, chunk), chunk), :].astype(jnp.float32)
        prod = cc[pl.ds(pl.multiple_of(source * chunk, chunk), chunk), :] * panel
        lane = prod[:, :128]
        for k in range(1, prod.shape[1] // 128):
            lane = lane + prod[:, k * 128 : (k + 1) * 128]
        return lax.dot_general(
            ones, lane, (((1,), (1,)), ((), ())),
            preferred_element_type=jnp.float32, precision=lax.Precision.HIGHEST,
        )

    def q_copy(p, source):
        return remote(qs.at[p], r1.at[source], q_send.at[0, p], q_recv.at[0, source], {"z": p})

    def sums_of(p):
        qs[p, :, :chunk] = part(p)
        q_copy(p, z).start()

    @pl.when(c == 0)
    def _():
        with jax.named_scope("p1a_wait"):

            @pl.loop(1, nz)
            def _(i):
                p = (z + i) % nz
                for core in range(2):
                    remote(ja.at[p], ra.at[core, p], p1_send.at[1, p], p1_recv.at[core, p], {"z": p, "c": 0}).wait_recv()

            remote(ja.at[z], ra.at[1, z], p1_send.at[1, z], p1_recv.at[1, z], {"z": z, "c": 1}).wait_recv()

        with jax.named_scope("repack"):
            repack(ra, ap.at[x, y])
        four(0, 0)
        four(1, 0)
        with jax.named_scope("four_x1"):
            four(0, 1)
            four(1, 1)
        with jax.named_scope("four_x2"):
            four(0, 2)
            four(2, 0)
            four(1, 2)
            four(3, 0)
        g_pass()
        with jax.named_scope("four_y1"):
            four(2, 1)
            four(3, 1)
        with jax.named_scope("four_y2"):
            four(2, 2)
            four(3, 2)
        g_whole()
        permute()
        multiply()
        b0 = bp.at[0, pl.ds(0, chunk), :]

        def take(p):
            ref = bp.at[p, pl.ds(0, chunk), :]
            remote(ref, ref, bd_send.at[p], bd_recv.at[p], {"c": 1 - c}).wait_recv()

        with jax.named_scope("parts"):
            take(z)
            r1[z, :, :chunk] = part(z)
            for step in range(1, far):
                for way in range(2):
                    p = source_of(way, step)
                    take(p)
                    sums_of(p)
            p = source_of(0, far)
            take(p)
        with jax.named_scope("part_last"):
            sums_of(p)

    @pl.when(c == 1)
    def _():
        with jax.named_scope("p1b_wait"):

            @pl.loop(1, NP)
            def _(i):
                p = (w + i) % NP
                for core in range(2):
                    remote(jb.at[p], rb.at[core, p], p1_send.at[0, p], p1_recv.at[core, p], dict(place(p), c=0)).wait_recv()

            remote(jb.at[w], rb.at[0, w], p1_send.at[0, w], p1_recv.at[0, w], {"c": 0}).wait_recv()

        with jax.named_scope("repack"):
            repack(rb, bp.at[z])
        ring_step(0)
        b_across(z).start()
        for step in range(1, 4):
            with jax.named_scope(f"ring_{step}"):
                ring_step(step)
        g_pass()
        for step in range(4, far):
            with jax.named_scope(f"ring_{step}"):
                ring_step(step)
        with jax.named_scope("a_wait"):
            g_whole()
            for kind in (2, 3):
                for source in range(4):
                    ref = unit(kind, source, chunk, chunk)
                    remote(ref, ref, ad_send.at[kind - 2, source], ad_recv.at[kind - 2, source], {"c": 1 - c}).wait_recv()
        permute()
        multiply()
        with jax.named_scope("parts"):
            r1[z, :, :chunk] = part(z)
            for step in range(1, far):
                for way in range(2):
                    sums_of(source_of(way, step))
        with jax.named_scope(f"ring_{far}"):
            ring_step(far)
        with jax.named_scope("part_last"):
            sums_of(source_of(0, far))

    with jax.named_scope("q1_wait"):

        @pl.loop(1, nz)
        def _(i):
            p = (z + i) % nz
            q_copy(p, p).wait_recv()

    s2[...] = jnp.sum(r1[...], axis=0)
    r2[w] = s2[...]

    def q2_copy(p, source):
        return remote(s2, r2.at[source], q_send.at[1, p], q_recv.at[1, source], place(p))

    @pl.loop(1, NP)
    def _(i):
        q2_copy((w + i) % NP, w).start()

    with jax.named_scope("q2_wait"):

        @pl.loop(1, NP)
        def _(i):
            p = (w + i) % NP
            q2_copy(p, p).wait_recv()

    sums = pltpu.roll(jnp.sum(r2[...], axis=0), 128 - w * rows, 1)
    out[...] = var[...] - sums[0:1, 0:rows]

    @pl.loop(1, NP)
    def _(i):
        p = (w + i) % NP
        first_b(p).wait_send()
        q2_copy(p, w).wait_send()

    @pl.loop(1, nz)
    def _(i):
        p = (z + i) % nz
        first_a(p).wait_send()
        q_copy(p, z).wait_send()

    @pl.loop(1, 8)
    def _(i):
        g_copy((own + i) % 8, own).wait_send()

    across.wait_send()

    @pl.when(c == 0)
    def _():
        first_b(w).wait_send()
        for kind in range(4):
            at = x if kind in (0, 3) else y
            for way in range(2):
                behind = (at + 3) % 4 if way == 0 else (at + 1) % 4
                mover(kind, way, 0, at).wait_send()
                mover(kind, way, 1, behind).wait_send()
        for kind in (2, 3):
            for source in range(4):
                a_across(kind, source).wait_send()

    @pl.when(c == 1)
    def _():
        first_a(z).wait_send()
        for step in range(far):
            for s in range(SUBS):
                for way in range(2):
                    if goes(way, step + 1, s):
                        ring_copy(way, step, s).wait_send()

        @pl.loop(0, nz)
        def _(p):
            b_across(p).wait_send()


def shards(jacobian, gain_inverse, variance):
    rows, states = jacobian.shape
    nz = lax.axis_size("z")
    chunk = rows * NP
    block = states // nz
    vmem = pl.BlockSpec(memory_space=pltpu.VMEM)
    dma = pltpu.SemaphoreType.DMA
    bf16, f32 = jnp.bfloat16, jnp.float32
    out = pl.pallas_call(
        functools.partial(kernel, nz, rows),
        out_shape=jax.ShapeDtypeStruct((1, rows), f32),
        in_specs=[vmem, vmem, pl.BlockSpec(memory_space=pl.ANY)],
        out_specs=vmem,
        scratch_shapes=[
            pltpu.VMEM((8 * rows * nz, 128), f32),
            pltpu.VMEM((8 * rows * NP, 128), f32),
            pltpu.VMEM((nz, 8 * rows, 128), bf16),
            pltpu.VMEM((NP, 8 * rows, 128), bf16),
            pltpu.VMEM((2, nz, 8 * rows, 128), bf16),
            pltpu.VMEM((2, NP, 8 * rows, 128), bf16),
            pltpu.VMEM((4, 4, 2 * chunk, block), bf16),
            pltpu.VMEM((nz * chunk, block), bf16),
            pltpu.VMEM((nz, 2 * chunk, block), bf16),
            pltpu.VMEM((block, block), bf16),
            pltpu.VMEM((nz * chunk, block), f32),
            pltpu.VMEM((nz * chunk, nz * chunk), bf16),
            pltpu.VMEM((nz, 8, 128), f32),
            pltpu.VMEM((nz, 8, 128), f32),
            pltpu.VMEM((8, 128), f32),
            pltpu.VMEM((NP, 8, 128), f32),
            dma((2, 16)),
            dma((2, 16)),
            dma((8,)),
            dma((8,)),
            dma((3,)),
            dma((2, nz // 2, SUBS)),
            dma((2, nz // 2, SUBS)),
            dma((4, 2, 2)),
            dma((4, 2, 2)),
            dma((2, 4)),
            dma((2, 4)),
            dma((16,)),
            dma((16,)),
            dma((2, 16)),
            dma((2, 16)),
        ],
        compiler_params=pltpu.CompilerParams(
            collective_id=0, has_side_effects=True, vmem_limit_bytes=48 * 1024 * 1024
        ),
    )(jacobian, variance.reshape(1, rows), gain_inverse)
    return out.reshape(rows)


def solution(mesh):
    split = Mesh(mesh.devices.reshape(2, 2, 16, 4, 2), AXES)
    return jax.shard_map(
        shards,
        mesh=split,
        in_specs=(P(AXES, None), P(("yh", "c"), ("z", "x", "yl")), P(AXES)),
        out_specs=P(AXES),
        check_vma=False,
    )
```
